32 devices in a mesh: items: 8 (over z, y), users: 4 (over x, core).
Axes of the slice: x: 2, y: 2, z: 4, core: 2. Of those that a mesh axis runs over, the one named last changes fastest.
Arguments:
- user_emb: bfloat16 [4096, 256], P('users', 'items'), as said below
- item_emb: bfloat16 [262144, 256], P('items'), as said below
- target: int32 [4096], P('users'), may hold values from 0 to 262143
- history: int32 [4096, 32], P('users'), may hold values from 0 to 262143, as said below
Outputs:
- log_rank: float32 [4096], P('users')
- metrics: float32 [2], replicated
The draws below stay inside these ranges and needn't reach their ends.
Inputs may be any that keep to these rules, and one draw needn't show every extreme that they name: history[u, k] lies in [k * 8192, (k + 1) * 8192); a user's history entries are thus distinct. `item_emb`: rows of norm about one. `user_emb`: entries of order one.
All inputs are finite; a program needn't handle non-finite values.
Results may differ from the reference program's by a relative error of at most 0.0003.
Values may be sent and summed in bfloat16 or wider, within the bound.
A program may use at most 64 MiB of HBM per device.

```python
import jax
import jax.numpy as jnp
from jax import lax

D = 256
H = 32
ITEMS = 262144
USERS = 4096


def item_row(base, row):
    return jax.random.normal(jax.random.fold_in(base, row), (D,), jnp.float32) / jnp.sqrt(float(D))


def shared_ints(key):
    target = jax.random.randint(jax.random.fold_in(key, 12), (USERS,), 0, ITEMS).astype(jnp.int32)
    stride = ITEMS // H
    offset = jax.random.randint(jax.random.fold_in(key, 13), (USERS, H), 0, stride).astype(jnp.int32)
    history = offset + (jnp.arange(H, dtype=jnp.int32) * stride)[None, :]
    return (target, history)


def draw_item_emb(key, part):
    base = jax.random.fold_in(key, 11)
    rows = jax.vmap(lambda r: item_row(base, r))(jnp.arange(ITEMS, dtype=jnp.int32))
    return rows.astype(jnp.bfloat16)


def draw_target(key, part):
    return shared_ints(key)[0]


def draw_history(key, part):
    return shared_ints(key)[1]


def draw_user_emb(key, part):
    base = jax.random.fold_in(key, 11)
    target, history = shared_ints(key)
    trow = jax.vmap(lambda r: item_row(base, r))(target)
    hrows = jax.vmap(jax.vmap(lambda r: item_row(base, r)))(history)
    noise = jax.random.normal(jax.random.fold_in(key, 14), (USERS, D), jnp.float32) * 0.6
    query = noise + 4.0 * trow + 2.5 * jnp.sum(hrows, axis=1)
    return query.astype(jnp.bfloat16)


def setup_inputs(seed: int = 0) -> dict:
    key_of = jax.random.split(jax.random.key(seed), 5)
    return {
        "user_emb": draw_user_emb(jax.random.fold_in(key_of[4], 71), 0),
        "item_emb": draw_item_emb(jax.random.fold_in(key_of[4], 71), 0),
        "target": draw_target(jax.random.fold_in(key_of[4], 71), 0),
        "history": draw_history(jax.random.fold_in(key_of[4], 71), 0),
    }


sharpness = 4.0


def reference(user_emb, item_emb, target, history):
    users = user_emb.astype(jnp.float32)
    items = item_emb.astype(jnp.float32)
    tscore = jnp.sum(users * items[target], axis=1)
    blk = min(ITEMS, 8192)
    nblk = ITEMS // blk
    blocks = items.reshape(nblk, blk, D)

    def step(total, rows):
        score = jnp.dot(users, rows.T, preferred_element_type=jnp.float32, precision=lax.Precision.HIGHEST)
        return total + jnp.sum(jax.nn.sigmoid(sharpness * (score - tscore[:, None])), axis=1), None

    total, _ = lax.scan(step, jnp.zeros((USERS,), jnp.float32), blocks)
    hrows = items[history]
    hscore = jnp.einsum("ud,uhd->uh", users, hrows, precision=lax.Precision.HIGHEST)
    seen_sum = jnp.sum(jax.nn.sigmoid(sharpness * (hscore - tscore[:, None])), axis=1)
    seen = jnp.any(history == target[:, None], axis=1)
    above = total - seen_sum - jnp.where(seen, 0.0, 0.5).astype(jnp.float32)
    rank = 1.0 + above
    log_rank = jnp.log(rank)
    hit = jax.nn.sigmoid(10.5 - rank)
    gain = hit / jnp.log2(1.0 + rank)
    metrics = jnp.stack([jnp.sum(hit), jnp.sum(gain)]) / USERS
    return log_rank, metrics
```

```python
import functools

import jax
import jax.numpy as jnp
from jax import lax
from jax.experimental import pallas as pl
from jax.experimental.pallas import tpu as pltpu
from jax.sharding import PartitionSpec as P

MESH = pl.DeviceIdType.MESH
CHUNK = 2048
GROUPS = 64
LOG_GROUPS = 6
SLOTS = 4
WIDTH = 512


def exchange(axis, n, me, src, dst, send, recv):
    copies = []
    for off in range(1, n):
        peer = lax.rem(me + off, n)
        copies.append(
            pltpu.make_async_remote_copy(
                src_ref=src,
                dst_ref=dst,
                send_sem=send.at[off - 1],
                recv_sem=recv.at[off - 1],
                device_id={axis: peer},
                device_id_type=MESH,
            )
        )
    for c in copies:
        c.start()
    return copies


def kernel(
    n, m, u_ref, own_ref, item_ref, tgt_ref, hist_ref, log_ref, met_ref,
    gath, w, buf, tpart, tslots, apart, aslots, mpart, mslots, tvec, acc,
    sem_item, sem_u, us, ur, ts, tr, as_, ar, ms, mr,
):
    me = lax.axis_index("items")
    grp = lax.axis_index("users")
    dsh, u_dev = u_ref.shape
    item_dev = item_ref.shape[0]
    n_chunks = item_dev // CHUNK
    per_shard = hist_ref.shape[0] // n
    span = item_dev // per_shard

    def fetch(i):
        return pltpu.make_async_copy(
            item_ref.at[pl.ds(i * CHUNK, CHUNK), :], buf.at[lax.rem(i, SLOTS)], sem_item.at[lax.rem(i, SLOTS)]
        )

    for i in range(min(SLOTS - 1, n_chunks)):
        fetch(i).start()
    mine = pl.ds(pl.multiple_of(me * dsh, dsh), dsh)
    keep = pltpu.make_async_copy(u_ref, gath.at[mine, :], sem_u)
    keep.start()

    barrier = pltpu.get_barrier_semaphore()
    for off in range(1, n):
        pl.semaphore_signal(barrier, inc=1, device_id={"items": lax.rem(me + off, n)}, device_id_type=MESH)
    for off in range(1, m):
        pl.semaphore_signal(barrier, inc=1, device_id={"users": lax.rem(grp + off, m)}, device_id_type=MESH)
    pl.semaphore_wait(barrier, n - 1 + m - 1)

    copies = exchange("items", n, me, u_ref, gath.at[mine, :], us, ur)
    keep.wait()
    for c in copies:
        c.wait()
    w[...] = gath[...] * jnp.bfloat16(2)

    step = 256
    eye = lax.broadcasted_iota(jnp.int32, (step, step), 0) == lax.broadcasted_iota(jnp.int32, (step, step), 1)
    for b in range(u_dev // step):
        cols = slice(b * step, (b + 1) * step)
        p = jnp.dot(own_ref[cols, :], w[:, cols], preferred_element_type=jnp.float32)
        p = jnp.sum(jnp.where(eye, p, 0.0), axis=0, keepdims=True)
        local = tgt_ref[:, cols] - me * item_dev
        inside = (local >= 0) & (local < item_dev)
        tpart[:, cols] = jnp.where(inside, p, 0.0)
    tslots[me] = tpart[...]
    copies = exchange("items", n, me, tpart, tslots.at[me], ts, tr)
    for c in copies:
        c.wait()
    tsum = tslots[0]
    for i in range(1, n):
        tsum = tsum + tslots[i]
    tvec[...] = jnp.broadcast_to(tsum, tvec.shape)
    acc[...] = jnp.zeros_like(acc)

    rows = GROUPS * 8
    iota8 = lax.broadcasted_iota(jnp.int32, (8, WIDTH), 0)

    def chunk(i, carry):
        fetch(i).wait()

        @pl.when(i + SLOTS - 1 < n_chunks)
        def _():
            fetch(i + SLOTS - 1).start()

        slot = lax.rem(i, SLOTS)
        k = lax.div(i * CHUNK, span)
        base = i * CHUNK - k * span
        row = me * per_shard + k
        for c in range(u_dev // WIDTH):
            cols = slice(c * WIDTH, (c + 1) * WIDTH)
            h = jnp.broadcast_to(hist_ref[pl.ds(row, 1), cols] - row * span, (8, WIDTH))
            t = tvec[:, cols]
            bits = [(h & (8 << b)) != 0 for b in range(LOG_GROUPS)]
            place = ((h >> (3 + LOG_GROUPS)) << 3) | (h & 7)
            total = acc[:, cols]
            for s in range(CHUNK // rows):
                part = jnp.dot(
                    buf[slot, pl.ds(s * rows, rows), :], w[:, cols], preferred_element_type=jnp.float32
                )
                sums, picks = [], []
                for g in range(GROUPS):
                    tau = jnp.tanh(part[8 * g : 8 * g + 8] - t)
                    lvl, v = 0, tau
                    while sums and sums[-1][0] == lvl:
                        v = sums.pop()[1] + v
                        lvl += 1
                    if lvl == 2:
                        total = total + (v + 4.0)
                    else:
                        sums.append((lvl, v))
                    lvl, v = 0, tau
                    while picks and picks[-1][0] == lvl:
                        v = jnp.where(bits[lvl], v, picks.pop()[1])
                        lvl += 1
                    picks.append((lvl, v))
                tile = lax.div(base, rows) + s
                match = place == iota8 + tile * 8
                total = total - jnp.where(match, picks[0][1] + 1.0, 0.0)
            acc[:, cols] = total
        return carry

    lax.fori_loop(0, n_chunks, chunk, 0)

    apart[...] = 0.5 * jnp.sum(acc[...], axis=0, keepdims=True)
    aslots[me] = apart[...]
    copies = exchange("items", n, me, apart, aslots.at[me], as_, ar)
    seen = jnp.max(jnp.where(hist_ref[...] == tgt_ref[...], 1.0, 0.0), axis=0, keepdims=True)
    for c in copies:
        c.wait()
    total = aslots[0]
    for i in range(1, n):
        total = total + aslots[i]
    rank = 1.0 + (total - jnp.where(seen > 0.5, 0.0, 0.5))
    log_ref[...] = jnp.log(rank)
    hit = jax.nn.sigmoid(10.5 - rank)
    gain = hit / jnp.log2(1.0 + rank)
    hs, gs = hit[:, :128], gain[:, :128]
    for b in range(1, u_dev // 128):
        hs = hs + hit[:, b * 128 : (b + 1) * 128]
        gs = gs + gain[:, b * 128 : (b + 1) * 128]
    mpart[:, :128] = hs
    mpart[:, 128:] = gs
    mslots[grp] = mpart[...]
    copies = exchange("users", m, grp, mpart, mslots.at[grp], ms, mr)
    for c in copies:
        c.wait()
    tot = mslots[0]
    for i in range(1, m):
        tot = tot + mslots[i]
    scale = 1.0 / (u_dev * m)
    met_ref[0] = jnp.sum(tot[:, :128]) * scale
    met_ref[1] = jnp.sum(tot[:, 128:]) * scale


def solution(mesh):
    n, m = mesh.shape["items"], mesh.shape["users"]

    def body(user_emb, item_emb, target, history):
        u_dev, dsh = user_emb.shape
        item_dev, d = item_emb.shape
        own = item_emb[jnp.remainder(target, item_dev)]
        vmem = pl.BlockSpec(memory_space=pltpu.VMEM)
        dma = pltpu.SemaphoreType.DMA
        log_rank, metrics = pl.pallas_call(
            functools.partial(kernel, n, m),
            out_shape=(
                jax.ShapeDtypeStruct((1, u_dev), jnp.float32),
                jax.ShapeDtypeStruct((2,), jnp.float32),
            ),
            in_specs=[vmem, vmem, pl.BlockSpec(memory_space=pl.ANY), vmem, vmem],
            out_specs=(vmem, pl.BlockSpec(memory_space=pltpu.SMEM)),
            scratch_shapes=[
                pltpu.VMEM((d, u_dev), jnp.bfloat16),
                pltpu.VMEM((d, u_dev), jnp.bfloat16),
                pltpu.VMEM((SLOTS, CHUNK, d), jnp.bfloat16),
                pltpu.VMEM((1, u_dev), jnp.float32),
                pltpu.VMEM((n, 1, u_dev), jnp.float32),
                pltpu.VMEM((1, u_dev), jnp.float32),
                pltpu.VMEM((n, 1, u_dev), jnp.float32),
                pltpu.VMEM((1, 256), jnp.float32),
                pltpu.VMEM((m, 1, 256), jnp.float32),
                pltpu.VMEM((8, u_dev), jnp.float32),
                pltpu.VMEM((8, u_dev), jnp.float32),
                dma((SLOTS,)),
                dma(()),
                dma((n - 1,)), dma((n - 1,)),
                dma((n - 1,)), dma((n - 1,)),
                dma((n - 1,)), dma((n - 1,)),
                dma((m - 1,)), dma((m - 1,)),
            ],
            compiler_params=pltpu.CompilerParams(
                collective_id=0, has_side_effects=True, vmem_limit_bytes=48 * 1024 * 1024
            ),
        )(user_emb.T, own, item_emb, target.reshape(1, u_dev), history.T)
        return log_rank.reshape(u_dev), metrics

    return jax.shard_map(
        body,
        mesh=mesh,
        in_specs=(P("users", "items"), P("items", None), P("users"), P("users", None)),
        out_specs=(P("users"), P()),
        check_vma=False,
    )
```

```python
import functools

import jax
import jax.numpy as jnp
from jax import lax
from jax.experimental import pallas as pl
from jax.experimental.pallas import tpu as pltpu
from jax.sharding import PartitionSpec as P

MESH = pl.DeviceIdType.MESH
CHUNK = 4096
GROUPS = 64
LOG_GROUPS = 6
WIDTH = 512
DOT = 512
PARTS = 2
PIECES = 8


def exchange(axis, n, me, src, dst, send, recv):
    copies = []
    for off in range(1, n):
        peer = lax.rem(me + off, n)
        copies.append(
            pltpu.make_async_remote_copy(
                src_ref=src,
                dst_ref=dst,
                send_sem=send.at[off - 1],
                recv_sem=recv.at[off - 1],
                device_id={axis: peer},
                device_id_type=MESH,
            )
        )
    for c in copies:
        c.start()
    return copies


def pick(tgt_ref, item_ref, own_ref, sem):
    item_dev = item_ref.shape[0]
    batch = 16

    def body(i, carry):
        for j in range(batch):
            user = i * batch + j
            local = lax.rem(tgt_ref[user], item_dev)
            row = pl.multiple_of((local >> 3) << 3, 8)
            pltpu.make_async_copy(
                item_ref.at[pl.ds(row, 8), :], own_ref.at[pl.ds(pl.multiple_of(user * 8, 8), 8), :], sem
            ).start()
        return carry

    u_dev = tgt_ref.shape[0]
    lax.fori_loop(0, u_dev // batch, body, 0)
    pltpu.make_async_copy(item_ref.at[pl.ds(0, u_dev * 8), :], own_ref, sem).wait()


def kernel(
    n, m, u_ref, own_ref, item_ref, tgt_ref, hist_ref, log_ref, met_ref,
    gath, w, items, own, tpart, tslots, apart, aslots, mpart, mslots, acc,
    sem_item, sem_own, sem_u, us, ur, ts, tr, as_, ar, ms, mr,
):
    me = lax.axis_index("items")
    grp = lax.axis_index("users")
    dsh, u_dev = u_ref.shape
    item_dev = item_ref.shape[0]
    per_shard = hist_ref.shape[0] // n
    span = item_dev // per_shard
    half = u_dev // PARTS
    piece = item_dev // PIECES

    fetches = []
    for i in range(PIECES):
        part = pl.ds(i * piece, piece)
        fetches.append(pltpu.make_async_copy(item_ref.at[part, :], items.at[part, :], sem_item.at[i]))
    mine = pl.ds(pl.multiple_of(me * dsh, dsh), dsh)
    keep = pltpu.make_async_copy(u_ref, gath.at[mine, :], sem_u)
    keep.start()
    tiles = pltpu.make_async_copy(own_ref, own, sem_own)
    tiles.start()
    for f in fetches:
        f.start()

    barrier = pltpu.get_barrier_semaphore()
    for off in range(1, n):
        pl.semaphore_signal(barrier, inc=1, device_id={"items": lax.rem(me + off, n)}, device_id_type=MESH)
    for off in range(1, m):
        pl.semaphore_signal(barrier, inc=1, device_id={"users": lax.rem(grp + off, m)}, device_id_type=MESH)
    pl.semaphore_wait(barrier, n - 1 + m - 1)

    ucopies = []
    for p in range(PARTS):
        cols = slice(p * half, (p + 1) * half)
        ucopies.append(exchange("items", n, me, u_ref.at[:, cols], gath.at[mine, cols], us.at[p], ur.at[p]))
    acc[...] = jnp.zeros_like(acc)
    keep.wait()
    tiles.wait()
    lane = lax.broadcasted_iota(jnp.int32, (8, 128), 1)
    sub = lax.broadcasted_iota(jnp.int32, (8, 128), 0)
    tcopies = []
    for p in range(PARTS):
        for c in ucopies[p]:
            c.wait()
        cols = slice(p * half, (p + 1) * half)
        w[:, cols] = gath[:, cols] * jnp.bfloat16(2)
        for b in range(half // 128):
            at = p * half + b * 128
            pc = jnp.dot(own[at * 8 : at * 8 + 1024, :], w[:, at : at + 128], preferred_element_type=jnp.float32)
            got = pc[:8]
            for r in range(1, 128):
                got = jnp.where(lane == r, pc[8 * r : 8 * r + 8], got)
            tgt = tgt_ref[:, at : at + 128]
            got = jnp.sum(jnp.where(sub == (tgt & 7), got, 0.0), axis=0, keepdims=True)
            local = tgt - me * item_dev
            tpart[p, :, b * 128 : (b + 1) * 128] = jnp.where((local >= 0) & (local < item_dev), got, 0.0)
        tslots[p, me] = tpart[p]
        tcopies.append(exchange("items", n, me, tpart.at[p], tslots.at[p, me], ts.at[p], tr.at[p]))

    rows = GROUPS * 8
    for f in fetches:
        f.wait()
    iota8 = lax.broadcasted_iota(jnp.int32, (8, WIDTH), 0)
    acopies = []
    for p in range(PARTS):
        for c in tcopies[p]:
            c.wait()
        tsum = tslots[p, 0]
        for i in range(1, n):
            tsum = tsum + tslots[p, i]
        tpart[p] = tsum

        def chunk(i, carry, p=p):
            k = lax.div(i * CHUNK, span)
            base = i * CHUNK - k * span
            row = me * per_shard + k
            for c in range(half // WIDTH):
                lo = p * half + c * WIDTH
                cols = slice(lo, lo + WIDTH)
                h = jnp.broadcast_to(hist_ref[pl.ds(row, 1), cols] - row * span, (8, WIDTH))
                t = jnp.broadcast_to(tpart[p, :, c * WIDTH : (c + 1) * WIDTH], (8, WIDTH))
                bits = [(h & (8 << b)) != 0 for b in range(LOG_GROUPS)]
                place = ((h >> (3 + LOG_GROUPS)) << 3) | (h & 7)
                total = acc[:, cols]
                for s in range(CHUNK // rows):
                    sums, picks = [], []
                    for q in range(rows // DOT):
                        at = pl.multiple_of(i * CHUNK + s * rows + q * DOT, DOT)
                        part = jnp.dot(items[pl.ds(at, DOT), :], w[:, cols], preferred_element_type=jnp.float32)
                        for g in range(DOT // 8):
                            tau = jnp.tanh(part[8 * g : 8 * g + 8] - t)
                            lvl, v = 0, tau
                            while sums and sums[-1][0] == lvl:
                                v = sums.pop()[1] + v
                                lvl += 1
                            if lvl == 2:
                                total = total + (v + 4.0)
                            else:
                                sums.append((lvl, v))
                            lvl, v = 0, tau
                            while picks and picks[-1][0] == lvl:
                                v = jnp.where(bits[lvl], v, picks.pop()[1])
                                lvl += 1
                            picks.append((lvl, v))
                    tile = lax.div(base, rows) + s
                    match = place == iota8 + tile * 8
                    total = total - jnp.where(match, picks[0][1] + 1.0, 0.0)
                acc[:, cols] = total
            return carry

        lax.fori_loop(0, item_dev // CHUNK, chunk, 0)
        cols = slice(p * half, (p + 1) * half)
        apart[p] = 0.5 * jnp.sum(acc[:, cols], axis=0, keepdims=True)
        aslots[p, me] = apart[p]
        acopies.append(exchange("items", n, me, apart.at[p], aslots.at[p, me], as_.at[p], ar.at[p]))

    seen = jnp.max(jnp.where(hist_ref[...] == tgt_ref[...], 1.0, 0.0), axis=0, keepdims=True)
    hs = jnp.zeros((1, 128), jnp.float32)
    gs = jnp.zeros((1, 128), jnp.float32)
    for p in range(PARTS):
        cols = slice(p * half, (p + 1) * half)
        for c in acopies[p]:
            c.wait()
        total = aslots[p, 0]
        for i in range(1, n):
            total = total + aslots[p, i]
        rank = 1.0 + (total - jnp.where(seen[:, cols] > 0.5, 0.0, 0.5))
        log_ref[:, cols] = jnp.log(rank)
        hit = jax.nn.sigmoid(10.5 - rank)
        gain = hit / jnp.log2(1.0 + rank)
        for b in range(half // 128):
            hs = hs + hit[:, b * 128 : (b + 1) * 128]
            gs = gs + gain[:, b * 128 : (b + 1) * 128]
    mpart[:, :128] = hs
    mpart[:, 128:] = gs
    mslots[grp] = mpart[...]
    copies = exchange("users", m, grp, mpart, mslots.at[grp], ms, mr)
    for c in copies:
        c.wait()
    tot = mslots[0]
    for i in range(1, m):
        tot = tot + mslots[i]
    scale = 1.0 / (u_dev * m)
    met_ref[0] = jnp.sum(tot[:, :128]) * scale
    met_ref[1] = jnp.sum(tot[:, 128:]) * scale


def solution(mesh):
    n, m = mesh.shape["items"], mesh.shape["users"]

    def body(user_emb, item_emb, target, history):
        u_dev, dsh = user_emb.shape
        item_dev, d = item_emb.shape
        half = u_dev // PARTS
        vmem = pl.BlockSpec(memory_space=pltpu.VMEM)
        hbm = pl.BlockSpec(memory_space=pltpu.HBM)
        dma = pltpu.SemaphoreType.DMA
        own = pl.pallas_call(
            pick,
            out_shape=jax.ShapeDtypeStruct((u_dev * 8, d), jnp.bfloat16),
            in_specs=[pl.BlockSpec(memory_space=pltpu.SMEM), pl.BlockSpec(memory_space=pltpu.HBM)],
            out_specs=vmem,
            scratch_shapes=[dma(())],
        )(target, item_emb)
        log_rank, metrics = pl.pallas_call(
            functools.partial(kernel, n, m),
            out_shape=(
                jax.ShapeDtypeStruct((1, u_dev), jnp.float32),
                jax.ShapeDtypeStruct((2,), jnp.float32),
            ),
            in_specs=[vmem, hbm, hbm, vmem, vmem],
            out_specs=(vmem, pl.BlockSpec(memory_space=pltpu.SMEM)),
            scratch_shapes=[
                pltpu.VMEM((d, u_dev), jnp.bfloat16),
                pltpu.VMEM((d, u_dev), jnp.bfloat16),
                pltpu.VMEM((item_dev, d), jnp.bfloat16),
                pltpu.VMEM((u_dev * 8, d), jnp.bfloat16),
                pltpu.VMEM((PARTS, 1, half), jnp.float32),
                pltpu.VMEM((PARTS, n, 1, half), jnp.float32),
                pltpu.VMEM((PARTS, 1, half), jnp.float32),
                pltpu.VMEM((PARTS, n, 1, half), jnp.float32),
                pltpu.VMEM((1, 256), jnp.float32),
                pltpu.VMEM((m, 1, 256), jnp.float32),
                pltpu.VMEM((8, u_dev), jnp.float32),
                dma((PIECES,)),
                dma(()),
                dma(()),
                dma((PARTS, n - 1)), dma((PARTS, n - 1)),
                dma((PARTS, n - 1)), dma((PARTS, n - 1)),
                dma((PARTS, n - 1)), dma((PARTS, n - 1)),
                dma((m - 1,)), dma((m - 1,)),
            ],
            compiler_params=pltpu.CompilerParams(
                collective_id=0, has_side_effects=True, vmem_limit_bytes=56 << 20
            ),
        )(user_emb.T, own, item_emb, target.reshape(1, u_dev), history.T)
        return log_rank.reshape(u_dev), metrics

    return jax.shard_map(
        body,
        mesh=mesh,
        in_specs=(P("users", "items"), P("items", None), P("users"), P("users", None)),
        out_specs=(P("users"), P()),
        check_vma=False,
    )
```
